32 devices in a mesh: wide: 16 (over z, y, x), narrow: 2 (over core).
Axes of the slice: x: 2, y: 2, z: 4, core: 2. Of those that a mesh axis runs over, the one named last changes fastest.
Arguments:
- tokens: bfloat16 [2048, 2048], P('wide'), may hold values from -6 to 6
- expert_ids: int32 [2048, 6], P('wide'), may hold values from 0 to 15, all different within a row; in each aligned block of 128 rows (0 to 127, 128 to 255, ...) at most 64 rows name the same one
- gate_weights: float32 [2048, 6], P('wide'), may hold values from 0.05 to 0.6
- shared_gate: bfloat16 [2048, 2816], P('wide', 'narrow'), may hold values from -0.125 to 0.125
- shared_up: bfloat16 [2048, 2816], P('wide', 'narrow'), may hold values from -0.125 to 0.125
- shared_down: bfloat16 [2816, 2048], P('narrow', 'wide'), may hold values from -0.109375 to 0.109375
- expert_gate: bfloat16 [16, 2048, 1408], P('wide', None, 'narrow'), may hold values from -0.125 to 0.125
- expert_up: bfloat16 [16, 2048, 1408], P('wide', None, 'narrow'), may hold values from -0.125 to 0.125
- expert_down: bfloat16 [16, 1408, 2048], P('wide', 'narrow'), may hold values from -0.15625 to 0.15625
Outputs:
- moe_out: bfloat16 [2048, 2048], P('wide', 'narrow')
The draws below stay inside these ranges and needn't reach their ends.
Inputs may be any that keep to these rules, and one draw needn't show every extreme that they name: `expert_ids`: the 6 ids of a row differ. Among the 128 rows of one index of wide, no expert is named by more than 64 rows.
All inputs are finite; a program needn't handle non-finite values.
Results may differ from the reference program's by a relative error of at most 0.0075.
Values may be sent and summed in bfloat16 or wider, within the bound.
A program may use at most 128 MiB of HBM per device.

```python
import math
import jax
import jax.numpy as jnp
import numpy as np
from jax import lax

D = 2048
MF = 1408
FS = 2816
TOP = 6
TOK_DEV = 128
EXPERTS = 16
TOKENS = 2048
CAP = 64
N_WIDE = 16
N_NARROW = 2


def block_scale(stream_key, dims, split, low, high):
    def one(axis_at, blocks):
        steps = jax.random.uniform(jax.random.fold_in(jax.random.fold_in(stream_key, 6), axis_at), (blocks,), jnp.float32, low / len(split), high / len(split))
        return jnp.repeat(jnp.exp(steps), dims[axis_at] // blocks).reshape((-1,) + (1,) * (len(dims) - axis_at - 1))

    factor_of = one(*split[0])
    for cut in split[1:]:
        factor_of = factor_of * one(*cut)
    return factor_of


def shared_out(rng, own, number, rows, number_of, top, most, slope):
    ranking = jax.random.permutation(rng, number_of)
    packed, usual = load_shares(number_of, rows * top, most, slope, True), load_shares(number_of, rows * top, most, slope, False)
    places = jnp.arange(number_of)

    def named(lengths, offset_by):
        used = int((lengths > 0).sum())
        fixed = max(1, used // 4)
        passed = fixed + (places - fixed + offset_by * (used - fixed)) % max(1, number_of - fixed)
        return jnp.zeros((number_of,), jnp.int32).at[ranking[jnp.where(places < fixed, places, passed)]].set(jnp.asarray(lengths, jnp.int32))

    lengths = jnp.where(number % 4 == 0, named(packed, number // 4), named(usual, number - number // 4 - 1))
    mixed = jax.random.permutation(jax.random.fold_in(own, 3), number_of)
    donor, receiver = mixed[0:number_of // 2 * 2:2], mixed[1:number_of // 2 * 2:2]
    margin = jnp.minimum(lengths[donor] - 1, most - lengths[receiver]) // 2
    margin = jnp.where((donor == ranking[0]) | (receiver == ranking[0]) | (lengths[receiver] == 0), 0, jnp.maximum(margin, 0))
    passed = jax.random.randint(jax.random.fold_in(own, 4), (number_of // 2,), 0, 1 << 20) % (margin + 1)
    lengths = lengths.at[donor].add(-passed).at[receiver].add(passed)
    labels = jnp.searchsorted(jnp.cumsum(lengths), jnp.arange(rows * top), side="right").astype(jnp.int32)
    listing = labels.reshape(top, rows).T
    listing = listing[jax.random.permutation(jax.random.fold_in(own, 1), rows)]
    offset_by = jax.random.randint(jax.random.fold_in(own, 2), (rows, 1), 0, top)
    return jnp.take_along_axis(listing, (jnp.arange(top)[None, :] + offset_by) % top, axis=1)


def load_shares(amount, total, limit, lean, full):
    portions = [(1 << 20) // math.isqrt(grade ** lean) + 1 for grade in range(1, amount + 1)]
    largest = limit if full else min(limit, max(-(-total // amount), total * portions[0] // sum(portions)))
    least = 1 if total - largest >= amount - 1 else 0
    counts, surplus = [largest] + [least] * (amount - 1), total - largest - least * (amount - 1)
    while surplus > 0:
        candidates = [i for i in range(1, amount) if counts[i] < largest] or [i for i in range(1, amount) if counts[i] < limit]
        whole, budget = sum([portions[i] for i in candidates]), surplus
        for i in candidates:
            more = min(limit - counts[i], max(1, budget * portions[i] // whole), surplus)
            counts[i] = counts[i] + more
            surplus = surplus - more
    return np.array(counts)


def normal_values(stream_key, extent, spread, reach, cuts=(), held_as=jnp.bfloat16):
    array = jax.random.normal(stream_key, extent, jnp.float32) * spread
    if len(cuts) > 0:
        array = block_scale(stream_key, extent, cuts, -0.22, 0.18) * array
    return jnp.clip(array, min=-reach, max=reach).astype(held_as)


def setup_inputs(seed: int = 0) -> dict:
    keys = jax.random.split(jax.random.key(seed), 10)
    tokens = normal_values(keys[0], (TOKENS, D), 1.0, 6.0, ((0, 16),))
    expert_ids_keys = jax.random.split(jax.random.fold_in(keys[1], 1), TOKENS // TOK_DEV)
    expert_ids_turns = jax.random.permutation(jax.random.fold_in(keys[1], 3), TOKENS // TOK_DEV)
    expert_ids = jax.vmap(lambda own, number: shared_out(jax.random.fold_in(keys[1], 2), own, number, TOK_DEV, EXPERTS, TOP, CAP, 2))(expert_ids_keys, expert_ids_turns).reshape((TOKENS, TOP))
    gate_weights = jnp.clip(jnp.exp(math.log(0.6) - 2.4849067 * jax.random.uniform(keys[2], (TOKENS, TOP), jnp.float32) ** block_scale(keys[2], (TOKENS, TOP), ((0, 16),), -0.2, 0.2)), 0.05, 0.6)
    shared_gate = normal_values(keys[3], (D, FS), D ** -0.5, 0.125, ((0, 16), (1, 2)))
    shared_up = normal_values(keys[4], (D, FS), D ** -0.5, 0.125, ((0, 16), (1, 2)))
    shared_down = normal_values(keys[5], (FS, D), FS ** -0.5, 0.109375, ((0, 2), (1, 16)))
    expert_gate = normal_values(keys[6], (EXPERTS, D, MF), D ** -0.5, 0.125, ((0, 16), (2, 2)))
    expert_up = normal_values(keys[7], (EXPERTS, D, MF), D ** -0.5, 0.125, ((0, 16), (2, 2)))
    expert_down = normal_values(keys[8], (EXPERTS, MF, D), MF ** -0.5, 0.15625, ((0, 16), (1, 2)))
    return {"tokens": tokens, "expert_ids": expert_ids, "gate_weights": gate_weights, "shared_gate": shared_gate, "shared_up": shared_up, "shared_down": shared_down, "expert_gate": expert_gate, "expert_up": expert_up, "expert_down": expert_down}


def expert_rows(rows_in, w_gate, w_up, w_down):
    gate_part = jnp.dot(rows_in, w_gate, preferred_element_type=jnp.float32)
    up_part = jnp.dot(rows_in, w_up, preferred_element_type=jnp.float32)
    hidden = (jax.nn.silu(gate_part) * up_part).astype(jnp.bfloat16)
    quarter = MF // N_NARROW
    summed = jnp.zeros((rows_in.shape[0], w_down.shape[1]), jnp.float32)
    for slice_idx in range(N_NARROW):
        lower = slice_idx * quarter
        partial_value = jnp.dot(hidden[:, lower:lower + quarter], w_down[lower:lower + quarter], preferred_element_type=jnp.float32)
        summed = summed + partial_value.astype(jnp.bfloat16).astype(jnp.float32)
    return summed.astype(jnp.bfloat16)


def reference(tokens, expert_ids, gate_weights, shared_gate, shared_up, shared_down, expert_gate, expert_up, expert_down):
    shared_g = jnp.dot(tokens, shared_gate, preferred_element_type=jnp.float32)
    shared_u = jnp.dot(tokens, shared_up, preferred_element_type=jnp.float32)
    shared_hidden = (jax.nn.silu(shared_g) * shared_u).astype(jnp.bfloat16)
    shared = jnp.dot(shared_hidden, shared_down, preferred_element_type=jnp.float32)
    slot_count = N_WIDE * CAP
    positions = jnp.arange(TOKENS, dtype=jnp.int32)

    def one_expert(routed, inputs):
        expert_index, w_gate, w_up, w_down = inputs
        matches = expert_ids == expert_index
        chosen = jnp.any(matches, axis=1)
        weight = jnp.sum(jnp.where(matches, gate_weights, jnp.float32(0.0)), axis=1)
        rank_pos = (jnp.cumsum(chosen.astype(jnp.int32)) - 1).astype(jnp.int32)
        target = jnp.where(chosen, rank_pos, slot_count).astype(jnp.int32)
        picked = jnp.zeros((slot_count + 1,), jnp.int32).at[target].set(positions)[:slot_count]
        weight_live = jnp.zeros((slot_count + 1,), jnp.float32).at[target].set(weight)[:slot_count]
        outputs = expert_rows(tokens[picked], w_gate, w_up, w_down)
        routed = routed.at[picked].add(weight_live[:, None] * outputs.astype(jnp.float32))
        return routed, None

    routed0 = jnp.zeros((TOKENS, D), jnp.float32)
    indices = jnp.arange(EXPERTS, dtype=jnp.int32)
    routed, unused = lax.scan(one_expert, routed0, (indices, expert_gate, expert_up, expert_down))
    return (shared + routed).astype(jnp.bfloat16)
```

```python
import functools

import jax
import jax.numpy as jnp
from jax import lax
from jax.experimental import pallas as pl
from jax.experimental.pallas import tpu as pltpu
from jax.sharding import PartitionSpec as P


def expert_ffn(received, w_gate, w_up, w_down):
    senders, items, width = received.shape
    flat_rows = received.reshape(senders * items, width)
    gate_part = jnp.dot(flat_rows, w_gate, preferred_element_type=jnp.float32)
    up_part = jnp.dot(flat_rows, w_up, preferred_element_type=jnp.float32)
    hidden = (jax.nn.silu(gate_part) * up_part).astype(jnp.bfloat16)
    partial_value = jnp.dot(hidden, w_down, preferred_element_type=jnp.float32).astype(jnp.bfloat16)
    return partial_value.reshape(senders, items, w_down.shape[1])


def dispatch_body(
    tokens,
    expert_ids,
    gate_weights,
    shared_gate,
    shared_up,
    shared_down,
    expert_gate,
    expert_up,
    expert_down,
):
    tok_count, width = tokens.shape
    top_count = expert_ids.shape[1]
    experts = lax.axis_size("wide") * expert_gate.shape[0]
    capacity = min(tok_count, 4 * tok_count * top_count // (3 * experts))
    narrow_count = lax.axis_size("narrow")
    w_gate = expert_gate[0]
    w_up = expert_up[0]
    w_down = expert_down[0]
    pairs = tok_count * top_count
    flat_ids = expert_ids.reshape(pairs)
    onehot = (flat_ids[:, None] == jnp.arange(experts, dtype=jnp.int32)[None, :]).astype(jnp.int32)
    before = jnp.cumsum(onehot, axis=0) - onehot
    slot_pos = jnp.sum(before * onehot, axis=1)
    target_slot = flat_ids * capacity + slot_pos
    source = (
        jnp.full((experts * capacity,), -1, jnp.int32)
        .at[target_slot]
        .set(jnp.arange(pairs, dtype=jnp.int32))
    )
    filled = source >= 0
    token_of = jnp.where(filled, source // top_count, 0)
    outgoing = jnp.where(filled[:, None], tokens[token_of], jnp.zeros((), jnp.bfloat16))
    outgoing = outgoing.reshape(experts, capacity, width)
    quarter = capacity // narrow_count
    own_rows = lax.dynamic_slice_in_dim(outgoing, lax.axis_index("narrow") * quarter, quarter, 1)
    arrived = lax.all_to_all(own_rows, "wide", split_axis=0, concat_axis=0, tiled=True)
    joined = lax.all_gather(arrived, "narrow", axis=1, tiled=True)
    partial_value = expert_ffn(joined, w_gate, w_up, w_down)
    expert_out = (
        lax.psum_scatter(partial_value, "narrow", scatter_dimension=2, tiled=True)
        .astype(jnp.float32)
        .astype(jnp.bfloat16)
    )
    returned = lax.all_to_all(expert_out, "wide", split_axis=0, concat_axis=0, tiled=True)
    returned_rows = returned.reshape(experts * capacity, returned.shape[2])
    pair_rows = returned_rows[target_slot].astype(jnp.float32)
    weighted = gate_weights.reshape(pairs, 1) * pair_rows
    routed = jnp.sum(weighted.reshape(tok_count, top_count, returned.shape[2]), axis=1)
    gate_sum = jnp.dot(
        tokens,
        lax.all_gather(shared_gate, "wide", axis=0, tiled=True),
        preferred_element_type=jnp.float32,
    )
    up_sum = jnp.dot(
        tokens,
        lax.all_gather(shared_up, "wide", axis=0, tiled=True),
        preferred_element_type=jnp.float32,
    )
    shared_hidden = (jax.nn.silu(gate_sum) * up_sum).astype(jnp.bfloat16)
    shared_terms = jnp.dot(
        shared_hidden,
        lax.all_gather(shared_down, "wide", axis=1, tiled=True),
        preferred_element_type=jnp.float32,
    )
    shared = lax.psum_scatter(shared_terms, "narrow", scatter_dimension=1, tiled=True)
    return (shared + routed).astype(jnp.bfloat16)


MESH = pl.DeviceIdType.MESH
ANY = pl.BlockSpec(memory_space=pl.ANY)
VMEM = pl.BlockSpec(memory_space=pltpu.VMEM)
LANES = 128
PLANE = 4


def plan(tok_count, top_count, experts, wide_count):
    capacity = min(tok_count, 4 * tok_count * top_count // (3 * experts))
    return capacity, wide_count == PLANE**2 and wide_count * tok_count <= 4 * experts * capacity


def homes(wide, pieces, core):
    lines = wide // PLANE
    order = []
    for turn in range(PLANE):
        for z in range(lines):
            spot = (turn, PLANE - 1 - turn)[(z + core) % 2]
            order.append(PLANE * (z if core else lines - 1 - z) + spot)
    return order[:pieces]


def piece_table(wide, pieces, core, chip):
    bits = pieces.bit_length()
    per = 30 // bits
    words = []
    for which in range(2):
        held = homes(wide, pieces, which)
        row = [held.index(j) if j in held else pieces for j in range(wide)]
        words.append(
            [
                sum(v << (bits * i) for i, v in enumerate(row[at : at + per]))
                for at in range(0, wide, per)
            ]
        )
    word = jnp.int32(0)
    for i, (low, high) in enumerate(zip(*words)):
        word = jnp.where(chip // per == i, jnp.where(core == 0, low, high), word)
    return (word >> (bits * (chip % per))) & ((1 << bits) - 1)


def greet(devices):
    barrier = pltpu.get_barrier_semaphore()
    for device in devices:
        pl.semaphore_signal(barrier, inc=1, device_id=device, device_id_type=MESH)
    pl.semaphore_wait(barrier, len(devices))


def fused_kernel(
    wide,
    slots,
    tok,
    ids,
    gains,
    gate,
    up,
    down,
    w_gate_in,
    w_up_in,
    w_down_in,
    out,
    every,
    all_in,
    all_ids,
    all_gains,
    w_gate,
    w_up,
    w_out,
    rows,
    slot_w,
    both,
    other,
    acc,
    twin_in,
    diag_in,
    side_in,
    line_in,
    send,
    recv,
    local,
):
    f32, bf16 = jnp.float32, jnp.bfloat16
    me = lax.axis_index("wide")
    core = lax.axis_index("narrow")
    lines = wide // PLANE
    count = tok.shape[0]
    share = count // 2
    half = share // 2
    pieces = gate.shape[1] // LANES
    my_piece = piece_table(wide, pieces, core, me)
    greet([(me ^ k, core) for k in range(1, wide)] + [(me, 1 - core)])
    x_peer, y_peer, twin = (me ^ 1, core), (me ^ 2, core), (me, 1 - core)
    plane = me // PLANE
    inner = (plane > 0) & (plane < lines - 1)
    started = []
    inner_started = []
    outer_started = []

    def copy(number, source, target, device, sent=None):
        return pltpu.make_async_remote_copy(
            src_ref=source,
            dst_ref=target,
            send_sem=send.at[number if sent is None else sent],
            recv_sem=recv.at[number],
            device_id=device,
            device_id_type=MESH,
        )

    def start(item):
        item.start()
        started.append(item)

    def start_inner(item):
        inner_started.append(item)

        @pl.when(inner)
        def _():
            item.start()

    def landed(number, place):
        copy(number, place, place, twin).wait_recv()

    def region(k, side=None, of=core):
        begin = k * count + of * share
        if side is None:
            return every.at[pl.ds(pl.multiple_of(begin, share), share)]
        return every.at[pl.ds(pl.multiple_of(begin + side * half, half), half)]

    Z, X, Y, XD, YD, T = (lines * i for i in range(6))
    W = T + 5 * lines
    G = W + 3 * wide
    R = G + 2 * wide
    E = R + wide + 4 * lines + 5

    def arrive(number, place):
        landed(number, place)
        start(copy(T + number, place, place, twin))

    def joined(number, k, side=None):
        landed(T + number, region(k, side, 1 - core))

    own = pltpu.make_async_copy(tok, every.at[pl.ds(0, count)], local.at[0])
    own.start()
    mine = tok.at[pl.ds(pl.multiple_of(core * share, share), share)]
    near, far = (me ^ PLANE, core), (me ^ (3 * PLANE), core)
    start(copy(X, mine, region(1), x_peer))
    start(copy(Y, mine, region(2), y_peer))
    start(copy(Z + 1, mine, region(PLANE), near))
    start_inner(copy(Z + 3, mine, region(3 * PLANE), far, E))
    for k in range(1, wide):
        start(copy(G + k, ids, all_ids.at[k], (me ^ k, core)))
        start(copy(G + wide + k, gains, all_gains.at[k], (me ^ k, core)))
    loads = [
        pltpu.make_async_copy(ids, all_ids.at[0], local.at[1]),
        pltpu.make_async_copy(gains, all_gains.at[0], local.at[8]),
    ]
    w_down = w_out.at[pl.ds(LANES, w_down_in.shape[0])]
    for number, (source, target) in enumerate(
        ((w_gate_in, w_gate), (w_up_in, w_up), (w_down_in, w_down))
    ):
        loads.append(pltpu.make_async_copy(source, target, local.at[5 + number]))
    for item in loads:
        item.start()

    def places(chip):
        at = pl.ds(pl.multiple_of(chip * LANES, LANES), LANES)
        return (
            all_in.at[at, pl.ds(0, LANES)],
            all_in.at[at, pl.ds(LANES, LANES)],
            w_out.at[pl.ds(0, LANES), at],
        )

    def parts(piece):
        piece = jnp.minimum(piece, pieces - 1)
        part = pl.ds(pl.multiple_of(piece * LANES, LANES), LANES)
        return (gate.at[:, part], up.at[:, part], down.at[part])

    def shared_copies(k):
        piece = piece_table(wide, pieces, core, me ^ k)
        return [
            copy(W + k + i * wide, source, target, (me ^ k, core))
            for i, (source, target) in enumerate(zip(parts(piece), places(me)))
        ]

    def send_shared(ks):
        for k in ks:

            @pl.when(piece_table(wide, pieces, core, me ^ k) < pieces)
            def _():
                for item in shared_copies(k):
                    item.start()

    def stage(d):
        landed(Z + d, region(PLANE * d))

    def spread(d):
        place = region(PLANE * d)
        start(copy(X + d, place, region((PLANE * d) ^ 1), x_peer))
        start(copy(Y + d, place, region((PLANE * d) ^ 2), y_peer))
        start(copy(T + Z + d, place, place, twin))

    def spread_if(where, d):
        place = region(PLANE * d)
        items = [
            copy(X + d, place, region((PLANE * d) ^ 1), x_peer),
            copy(Y + d, place, region((PLANE * d) ^ 2), y_peer),
            copy(T + Z + d, place, place, twin),
        ]

        @pl.when(where)
        def _():
            for item in items:
                item.start()

    def beside(d):
        k = 1 ^ (PLANE * d)
        arrive(X + d, region(k))
        start(copy(YD + d, region(k, 1), region(k ^ 2, 1), y_peer))
        k = 2 ^ (PLANE * d)
        arrive(Y + d, region(k))
        start(copy(XD + d, region(k, 0), region(k ^ 1, 0), x_peer))

    def corner(d):
        k = 3 ^ (PLANE * d)
        arrive(XD + d, region(k, 0))
        arrive(YD + d, region(k, 1))

    lane_r = lax.broadcasted_iota(jnp.int32, (count, count), 0)
    lane_c = lax.broadcasted_iota(jnp.int32, (count, count), 1)
    upper = (lane_r <= lane_c).astype(f32).astype(bf16)
    slot = lax.broadcasted_iota(jnp.int32, (slots, count), 0).astype(f32)

    def across(a, b):
        return lax.dot_general(a, b, (((1,), (1,)), ((), ())), preferred_element_type=f32)

    def block(k):
        return pl.ds(pl.multiple_of(k * count, count), count)

    def routed(ks):
        picks = []
        for b, k in enumerate(ks):
            match = all_ids[k] == me
            value = jnp.sum(jnp.where(match, all_gains[k], 0.0), axis=0, keepdims=True)
            chosen = jnp.sum(match.astype(f32), axis=0, keepdims=True)
            chosen = jnp.broadcast_to(chosen, (8, count))
            rank = jnp.dot(chosen.astype(bf16), upper, preferred_element_type=f32)
            where = jnp.where(chosen > 0.0, rank - 1.0, -1.0)[0:1]
            pick = (jnp.broadcast_to(where, (slots, count)) == slot).astype(f32)
            picks.append(pick)
            place = pl.ds(b * slots, slots)
            slot_w[place] = jnp.sum(pick * value, axis=1, keepdims=True)
            rows[place] = jnp.dot(
                pick.astype(bf16), every[block(k)], preferred_element_type=f32
            ).astype(bf16)
        gate_part = across(rows[...], w_gate[...])
        up_part = across(rows[...], w_up[...])
        hidden = (jax.nn.silu(gate_part) * up_part * slot_w[...]).astype(bf16)
        for b, k in enumerate(ks):
            back = jnp.dot(
                picks[b].T.astype(bf16),
                hidden[b * slots : (b + 1) * slots],
                preferred_element_type=f32,
            )
            both[block(k), LANES:] = back.astype(bf16)

    width = out.shape[1]

    def partials(at):
        pre = jnp.dot(every[at], all_in[...], preferred_element_type=f32)
        both[at, :LANES] = (jax.nn.silu(pre[:, :LANES]) * pre[:, LANES:]).astype(bf16)
        for target, which in ((other, 1 - core), (acc, core)):
            columns = pl.ds(pl.multiple_of(which * width, width), width)
            part = jnp.dot(both[at], w_out[:, columns], preferred_element_type=f32)
            target[at] = part.astype(bf16)

    second = jnp.where(inner, 3, 2)
    third = 5 - second
    EARLY, MIDDLE = [], [12, 8, 13, 9, 14, 10, 15, 11]
    send_shared(EARLY)

    @pl.when(my_piece < pieces)
    def _():
        items = [
            pltpu.make_async_copy(source, target, local.at[2 + i])
            for i, (source, target) in enumerate(zip(parts(my_piece), places(me)))
        ]
        for item in items:
            item.start()
        for item in items:
            item.wait()

    @pl.when(my_piece >= pieces)
    def _():
        all_in[...] = jnp.zeros_like(all_in)
        w_out[0:LANES] = jnp.zeros((LANES, w_out.shape[1]), bf16)

    stage(1)
    start_inner(copy(Z + 2, region(PLANE), region(2 * PLANE), far, E + 1))
    spread(1)

    @pl.when(inner)
    def _():
        stage(3)
        copy(Z + 2, region(3 * PLANE), region(2 * PLANE), near, E + 2).start()

    spread_if(inner, 3)
    beside(0)
    for k in range(1, wide):
        landed(G + k, all_ids.at[k])
        landed(G + wide + k, all_gains.at[k])
    for item in loads:
        item.wait()
    own.wait()
    joined(Z + 1, PLANE)
    joined(X, 1)
    joined(Y, 2)
    routed([0, 1, 2, PLANE])

    @pl.when(jnp.logical_not(inner))
    def _():
        stage(2)

    spread_if(jnp.logical_not(inner), 2)
    beside(1)
    stage(third)
    start_inner(copy(Z + 3, region(2 * PLANE), region(3 * PLANE), near, E + 3))
    spread(third)
    send_shared(MIDDLE)
    corner(0)
    joined(Z + second, PLANE * second)
    joined(X + 1, PLANE ^ 1)
    joined(Y + 1, PLANE ^ 2)
    joined(XD, 3, 0)
    joined(YD, 3, 1)
    routed([PLANE * second, PLANE ^ 1, PLANE ^ 2, 3])
    beside(second)
    beside(third)
    send_shared([k for k in range(1, wide) if k not in EARLY + MIDDLE])
    corner(1)
    joined(Z + third, PLANE * third)
    joined(X + second, (PLANE * second) ^ 1)
    joined(Y + second, (PLANE * second) ^ 2)
    joined(XD + 1, 3 ^ PLANE, 0)
    joined(YD + 1, 3 ^ PLANE, 1)
    routed([PLANE * third, (PLANE * second) ^ 1, (PLANE * second) ^ 2, 3 ^ PLANE])
    corner(second)
    corner(third)
    joined(X + third, (PLANE * third) ^ 1)
    joined(Y + third, (PLANE * third) ^ 2)
    for d in (second, third):
        joined(XD + d, 3 ^ (PLANE * d), 0)
        joined(YD + d, 3 ^ (PLANE * d), 1)
    routed(
        [
            (PLANE * third) ^ 1,
            (PLANE * third) ^ 2,
            3 ^ (PLANE * second),
            3 ^ (PLANE * third),
        ]
    )
    for k in range(1, wide):

        @pl.when(my_piece < pieces)
        def _():
            for i, target in enumerate(places(me ^ k)):
                landed(W + k + i * wide, target)

    RT, RXD, RYD = R, R + wide, R + wide + lines
    RX, RY, RZ = RYD + lines, RYD + 2 * lines, RYD + 3 * lines
    step = 16

    def rows_of(ref, k, begin=0, size=count):
        return ref.at[pl.ds(k * count + begin, size)]

    def add(target, sources):
        def one(i, carry):
            at = pl.ds(pl.multiple_of(i * step, step), step)
            value = target[at].astype(f32)
            for source in sources:
                value += source[at].astype(f32)
            target[at] = value.astype(bf16)
            return carry

        lax.fori_loop(0, target.shape[0] // step, one, 0)

    def compute(d, flips):
        first = PLANE * d + flips[0]
        partials(pl.ds(first * count, len(flips) * count))
        for flip in flips:
            k = PLANE * d + flip
            start(copy(RT + k, rows_of(other, k), rows_of(twin_in, k), twin))

    def fold(k):
        landed(RT + k, rows_of(twin_in, k))
        add(rows_of(acc, k), [rows_of(twin_in, k)])

    tall = count // 2

    def diagonal(d):
        k = 3 ^ (PLANE * d)
        fold(k)
        start(copy(RXD + d, rows_of(acc, k, 0, tall), diag_in.at[0, d], x_peer))
        start(copy(RYD + d, rows_of(acc, k, tall, tall), diag_in.at[1, d], y_peer))

    def sides(d):
        k = 2 ^ (PLANE * d)
        fold(k)
        landed(RXD + d, diag_in.at[0, d])
        add(rows_of(acc, k, 0, tall), [diag_in.at[0, d]])
        start(copy(RY + d, rows_of(acc, k), side_in.at[1, d], y_peer))
        k = 1 ^ (PLANE * d)
        fold(k)
        landed(RYD + d, diag_in.at[1, d])
        add(rows_of(acc, k, tall, tall), [diag_in.at[1, d]])
        start(copy(RX + d, rows_of(acc, k), side_in.at[0, d], x_peer))

    near_in, far_in, far_out = line_in.at[0], line_in.at[1], line_in.at[2]

    def upright(d):
        k = PLANE * d
        fold(k)
        landed(RX + d, side_in.at[0, d])
        landed(RY + d, side_in.at[1, d])
        add(rows_of(acc, k), [side_in.at[0, d], side_in.at[1, d]])

    def outward(number, k, place):
        item = copy(RZ + number, rows_of(acc, k), place, near)
        outer_started.append(item)

        @pl.when(jnp.logical_not(inner))
        def _():
            item.start()

    def inward(number, place, k, item):
        inner_started.append(item)

        @pl.when(inner)
        def _():
            landed(RZ + number, place)
            add(rows_of(acc, k), [place])
            item.start()

    one, two, three = PLANE, 2 * PLANE, 3 * PLANE
    compute(3, [3])
    compute(2, [3])
    diagonal(3)
    compute(3, [1, 2])
    diagonal(2)
    compute(3, [0])
    compute(1, [3])
    sides(3)
    diagonal(1)
    compute(2, [1, 2])
    compute(2, [0])
    sides(2)
    upright(3)
    outward(0, three, near_in)
    compute(0, [3])
    diagonal(0)
    compute(1, [1, 2])
    sides(1)
    compute(1, [0])
    upright(2)
    outward(1, two, far_in)
    inward(0, near_in, two, copy(RZ + 2, rows_of(acc, two), far_out, far))
    compute(0, [1, 2])
    sides(0)
    compute(0, [0])
    inward(1, far_in, three, copy(RZ + 3, rows_of(acc, three), line_in.at[3], far))
    upright(1)
    outward(4, one, line_in.at[4])
    inward(2, far_out, one, copy(RZ + 4, rows_of(acc, one), line_in.at[4], near))
    upright(0)

    @pl.when(inner)
    def _():
        landed(RZ + 3, line_in.at[3])
        add(rows_of(acc, 0), [line_in.at[3]])

    landed(RZ + 4, line_in.at[4])

    def last(i, carry):
        at = pl.ds(pl.multiple_of(i * step, step), step)
        value = acc[at].astype(f32)
        out[at] = (value + line_in[4, at].astype(f32)).astype(bf16)
        return carry

    lax.fori_loop(0, count // step, last, 0)
    for k in range(1, wide):

        @pl.when(piece_table(wide, pieces, core, me ^ k) < pieces)
        def _():
            for item in shared_copies(k):
                item.wait_send()

    for item in started:
        item.wait_send()

    place = region(PLANE * second)
    copy(X + second, place, region((PLANE * second) ^ 1), x_peer).wait_send()
    copy(Y + second, place, region((PLANE * second) ^ 2), y_peer).wait_send()
    copy(T + Z + second, place, place, twin).wait_send()

    @pl.when(inner)
    def _():
        copy(Z + 2, region(3 * PLANE), region(2 * PLANE), near, E + 2).wait_send()
        for item in inner_started:
            item.wait_send()

    @pl.when(jnp.logical_not(inner))
    def _():
        for item in outer_started:
            item.wait_send()


def fused(wide, narrow, slots, tokens, ids, gains, gate, up, down, w_gate, w_up, w_down):
    count, width = tokens.shape
    part = width // narrow
    lines = wide // PLANE
    total = wide * count
    sems = 10 * lines + 6 * wide + 4 * lines + 5 + 4
    bf16, f32 = jnp.bfloat16, jnp.float32
    return pl.pallas_call(
        functools.partial(fused_kernel, wide, slots),
        out_shape=jax.ShapeDtypeStruct((count, part), bf16),
        in_specs=[VMEM] * 6 + [ANY] * 3,
        out_specs=VMEM,
        scratch_shapes=[
            pltpu.VMEM((total, width), bf16),
            pltpu.VMEM((wide * gate.shape[0], 2 * LANES), bf16),
            pltpu.VMEM((wide,) + ids.shape, jnp.int32),
            pltpu.VMEM((wide,) + gains.shape, f32),
            pltpu.VMEM(w_gate.shape, bf16),
            pltpu.VMEM(w_up.shape, bf16),
            pltpu.VMEM((LANES + w_down.shape[0], w_down.shape[1]), bf16),
            pltpu.VMEM((lines * slots, width), bf16),
            pltpu.VMEM((lines * slots, 1), f32),
            pltpu.VMEM((total, LANES + w_gate.shape[0]), bf16),
            pltpu.VMEM((total, part), bf16),
            pltpu.VMEM((total, part), bf16),
            pltpu.VMEM((total, part), bf16),
            pltpu.VMEM((2, lines, count // 2, part), bf16),
            pltpu.VMEM((2, lines, count, part), bf16),
            pltpu.VMEM((5, count, part), bf16),
            pltpu.SemaphoreType.DMA((sems,)),
            pltpu.SemaphoreType.DMA((sems,)),
            pltpu.SemaphoreType.DMA((9,)),
        ],
        compiler_params=pltpu.CompilerParams(
            collective_id=0, has_side_effects=True, vmem_limit_bytes=63 << 20
        ),
    )(tokens, ids, gains, gate, up, down, w_gate, w_up, w_down)


def gather_body(
    tokens,
    expert_ids,
    gate_weights,
    shared_gate,
    shared_up,
    shared_down,
    expert_gate,
    expert_up,
    expert_down,
):
    tok_count, top_count = expert_ids.shape
    wide = lax.axis_size("wide")
    narrow = lax.axis_size("narrow")
    experts = wide * expert_gate.shape[0]
    capacity, _ = plan(tok_count, top_count, experts, wide)
    return fused(
        wide,
        narrow,
        capacity,
        tokens,
        expert_ids.T,
        gate_weights.T,
        shared_gate,
        shared_up,
        shared_down,
        expert_gate[0].T,
        expert_up[0].T,
        expert_down[0],
    )


def solution(mesh):
    in_specs = (
        P("wide", None),
        P("wide", None),
        P("wide", None),
        P("wide", "narrow"),
        P("wide", "narrow"),
        P("narrow", "wide"),
        P("wide", None, "narrow"),
        P("wide", None, "narrow"),
        P("wide", "narrow", None),
    )
    out_specs = P("wide", "narrow")
    wide_count = mesh.shape["wide"]

    def body(*args):
        tok_count, top_count = args[1].shape
        gathers = plan(tok_count, top_count, wide_count * args[6].shape[0], wide_count)[1]
        return (gather_body if gathers else dispatch_body)(*args)

    return jax.shard_map(body, mesh=mesh, in_specs=in_specs, out_specs=out_specs, check_vma=False)
```

```python
import functools

import jax
import jax.numpy as jnp
from jax import lax
from jax.experimental import pallas as pl
from jax.experimental.pallas import tpu as pltpu
from jax.sharding import PartitionSpec as P


def expert_ffn(received, w_gate, w_up, w_down):
    senders, items, width = received.shape
    flat_rows = received.reshape(senders * items, width)
    gate_part = jnp.dot(flat_rows, w_gate, preferred_element_type=jnp.float32)
    up_part = jnp.dot(flat_rows, w_up, preferred_element_type=jnp.float32)
    hidden = (jax.nn.silu(gate_part) * up_part).astype(jnp.bfloat16)
    partial_value = jnp.dot(hidden, w_down, preferred_element_type=jnp.float32).astype(jnp.bfloat16)
    return partial_value.reshape(senders, items, w_down.shape[1])


def dispatch_body(
    tokens,
    expert_ids,
    gate_weights,
    shared_gate,
    shared_up,
    shared_down,
    expert_gate,
    expert_up,
    expert_down,
):
    tok_count, width = tokens.shape
    top_count = expert_ids.shape[1]
    experts = lax.axis_size("wide") * expert_gate.shape[0]
    capacity = min(tok_count, 4 * tok_count * top_count // (3 * experts))
    narrow_count = lax.axis_size("narrow")
    w_gate = expert_gate[0]
    w_up = expert_up[0]
    w_down = expert_down[0]
    pairs = tok_count * top_count
    flat_ids = expert_ids.reshape(pairs)
    onehot = (flat_ids[:, None] == jnp.arange(experts, dtype=jnp.int32)[None, :]).astype(jnp.int32)
    before = jnp.cumsum(onehot, axis=0) - onehot
    slot_pos = jnp.sum(before * onehot, axis=1)
    target_slot = flat_ids * capacity + slot_pos
    source = (
        jnp.full((experts * capacity,), -1, jnp.int32)
        .at[target_slot]
        .set(jnp.arange(pairs, dtype=jnp.int32))
    )
    filled = source >= 0
    token_of = jnp.where(filled, source // top_count, 0)
    outgoing = jnp.where(filled[:, None], tokens[token_of], jnp.zeros((), jnp.bfloat16))
    outgoing = outgoing.reshape(experts, capacity, width)
    quarter = capacity // narrow_count
    own_rows = lax.dynamic_slice_in_dim(outgoing, lax.axis_index("narrow") * quarter, quarter, 1)
    arrived = lax.all_to_all(own_rows, "wide", split_axis=0, concat_axis=0, tiled=True)
    joined = lax.all_gather(arrived, "narrow", axis=1, tiled=True)
    partial_value = expert_ffn(joined, w_gate, w_up, w_down)
    expert_out = (
        lax.psum_scatter(partial_value, "narrow", scatter_dimension=2, tiled=True)
        .astype(jnp.float32)
        .astype(jnp.bfloat16)
    )
    returned = lax.all_to_all(expert_out, "wide", split_axis=0, concat_axis=0, tiled=True)
    returned_rows = returned.reshape(experts * capacity, returned.shape[2])
    pair_rows = returned_rows[target_slot].astype(jnp.float32)
    weighted = gate_weights.reshape(pairs, 1) * pair_rows
    routed = jnp.sum(weighted.reshape(tok_count, top_count, returned.shape[2]), axis=1)
    gate_sum = jnp.dot(
        tokens,
        lax.all_gather(shared_gate, "wide", axis=0, tiled=True),
        preferred_element_type=jnp.float32,
    )
    up_sum = jnp.dot(
        tokens,
        lax.all_gather(shared_up, "wide", axis=0, tiled=True),
        preferred_element_type=jnp.float32,
    )
    shared_hidden = (jax.nn.silu(gate_sum) * up_sum).astype(jnp.bfloat16)
    shared_terms = jnp.dot(
        shared_hidden,
        lax.all_gather(shared_down, "wide", axis=1, tiled=True),
        preferred_element_type=jnp.float32,
    )
    shared = lax.psum_scatter(shared_terms, "narrow", scatter_dimension=1, tiled=True)
    return (shared + routed).astype(jnp.bfloat16)


MESH = pl.DeviceIdType.MESH
ANY = pl.BlockSpec(memory_space=pl.ANY)
VMEM = pl.BlockSpec(memory_space=pltpu.VMEM)
LANES = 128
PLANE = 4


def plan(tok_count, top_count, experts, wide_count):
    capacity = min(tok_count, 4 * tok_count * top_count // (3 * experts))
    return capacity, wide_count == PLANE**2 and wide_count * tok_count <= 4 * experts * capacity


def homes(wide, pieces, core):
    lines = wide // PLANE
    inner, edge, late = [], [], []
    for z in range(lines):
        pair = [PLANE * z + i for i in ((1, 2) if z % 2 else (0, 3))]
        if 0 < z < lines - 1:
            inner += pair
        else:
            edge.append(pair[0])
            late.append(pair[1])
    both = (inner + edge + late)[: max(0, 2 * pieces - wide)]
    single = [chip for chip in range(wide) if chip not in both]
    return (both + single[core::2])[:pieces]


def piece_table(wide, pieces, core, chip):
    bits = pieces.bit_length()
    per = 30 // bits
    words = []
    for which in range(2):
        held = homes(wide, pieces, which)
        row = [held.index(j) if j in held else pieces for j in range(wide)]
        words.append(
            [
                sum(v << (bits * i) for i, v in enumerate(row[at : at + per]))
                for at in range(0, wide, per)
            ]
        )
    word = jnp.int32(0)
    for i, (low, high) in enumerate(zip(*words)):
        word = jnp.where(chip // per == i, jnp.where(core == 0, low, high), word)
    return (word >> (bits * (chip % per))) & ((1 << bits) - 1)


def greet(devices):
    barrier = pltpu.get_barrier_semaphore()
    for device in devices:
        pl.semaphore_signal(barrier, inc=1, device_id=device, device_id_type=MESH)
    pl.semaphore_wait(barrier, len(devices))


def fused_kernel(
    wide,
    slots,
    tok,
    ids,
    gains,
    gate,
    up,
    down,
    w_gate_in,
    w_up_in,
    w_down_in,
    out,
    every,
    all_in,
    all_ids,
    all_gains,
    w_gate,
    w_up,
    w_out,
    rows,
    slot_w,
    both,
    other,
    acc,
    twin_in,
    diag_in,
    side_in,
    line_in,
    plane_in,
    send,
    recv,
    local,
):
    f32, bf16 = jnp.float32, jnp.bfloat16
    me = lax.axis_index("wide")
    core = lax.axis_index("narrow")
    lines = wide // PLANE
    count = tok.shape[0]
    share = count // 2
    half = share // 2
    pieces = gate.shape[1] // LANES
    my_piece = piece_table(wide, pieces, core, me)
    greet([(me ^ k, core) for k in range(1, wide)] + [(me, 1 - core)])
    x_peer, y_peer, twin = (me ^ 1, core), (me ^ 2, core), (me, 1 - core)
    plane = me // PLANE
    inner = (plane > 0) & (plane < lines - 1)
    started = []
    inner_started = []
    outer_started = []

    def copy(number, source, target, device, sent=None):
        return pltpu.make_async_remote_copy(
            src_ref=source,
            dst_ref=target,
            send_sem=send.at[number if sent is None else sent],
            recv_sem=recv.at[number],
            device_id=device,
            device_id_type=MESH,
        )

    def start(item):
        item.start()
        started.append(item)

    def start_inner(item):
        inner_started.append(item)

        @pl.when(inner)
        def _():
            item.start()

    def landed(number, place):
        copy(number, place, place, twin).wait_recv()

    def region(k, side=None, of=core, begin=0, size=None):
        first = k * count + of * share
        if size is not None:
            first, tile, size = first + begin, LANES // 8, size
        elif side is None:
            tile = size = share
        else:
            first, tile, size = first + side * half, half, half
        return every.at[pl.ds(pl.multiple_of(first, tile), size)]

    Z, X, Y, XD, YD, B = 0, 2 * lines, 4 * lines, 6 * lines, 7 * lines, 8 * lines
    T = 9 * lines
    W = 2 * T
    G = W + 3 * wide
    R = G + 2 * wide
    RC = R + wide + 4 * lines
    E = RC + 10 + 9

    def arrive(number, place):
        landed(number, place)
        start(copy(T + number, place, place, twin))

    def joined(number, place):
        landed(T + number, place)

    own = pltpu.make_async_copy(tok, every.at[pl.ds(0, count)], local.at[0])
    own.start()
    near, far = (me ^ PLANE, core), (me ^ (3 * PLANE), core)
    for h in range(2):
        mine = tok.at[pl.ds(pl.multiple_of(core * share + h * half, half), half)]
        start(copy(Z + 2 + h, mine, region(PLANE, h), near))
        start_inner(copy(Z + 6 + h, mine, region(3 * PLANE, h), far, E + h))
        start(copy(X + h, mine, region(1, h), x_peer))
        start(copy(Y + h, mine, region(2, h), y_peer))
    for k in range(1, wide):
        start(copy(G + k, ids, all_ids.at[k], (me ^ k, core)))
        start(copy(G + wide + k, gains, all_gains.at[k], (me ^ k, core)))
    loads = [
        pltpu.make_async_copy(ids, all_ids.at[0], local.at[1]),
        pltpu.make_async_copy(gains, all_gains.at[0], local.at[8]),
    ]
    w_down = w_out.at[pl.ds(LANES, w_down_in.shape[0])]
    for number, (source, target) in enumerate(
        ((w_gate_in, w_gate), (w_up_in, w_up), (w_down_in, w_down))
    ):
        loads.append(pltpu.make_async_copy(source, target, local.at[5 + number]))
    for item in loads:
        item.start()

    def places(chip):
        at = pl.ds(pl.multiple_of(chip * LANES, LANES), LANES)
        return (
            all_in.at[at, pl.ds(0, LANES)],
            all_in.at[at, pl.ds(LANES, LANES)],
            w_out.at[pl.ds(0, LANES), at],
        )

    def parts(piece):
        piece = jnp.minimum(piece, pieces - 1)
        part = pl.ds(pl.multiple_of(piece * LANES, LANES), LANES)
        return (gate.at[:, part], up.at[:, part], down.at[part])

    def shared_copies(k):
        piece = piece_table(wide, pieces, core, me ^ k)
        return [
            copy(W + k + i * wide, source, target, (me ^ k, core))
            for i, (source, target) in enumerate(zip(parts(piece), places(me)))
        ]

    def send_shared(ks):
        for k in ks:

            @pl.when(piece_table(wide, pieces, core, me ^ k) < pieces)
            def _():
                for item in shared_copies(k):
                    item.start()

    def onward(d, h):
        place = region(PLANE * d, h)
        return [
            copy(X + 2 * d + h, place, region((PLANE * d) ^ 1, h), x_peer),
            copy(Y + 2 * d + h, place, region((PLANE * d) ^ 2, h), y_peer),
            copy(T + Z + 2 * d + h, place, place, twin),
        ]

    def stage(d, h):
        landed(Z + 2 * d + h, region(PLANE * d, h))

    def stage_if(where, d, h, then=()):
        @pl.when(where)
        def _():
            stage(d, h)
            for item in list(then) + onward(d, h):
                item.start()

    def spread(d, h):
        for item in onward(d, h):
            start(item)

    def corner_rows(d, side):
        if isinstance(d, int) and d == 1:
            return {"begin": side * (half // 2), "size": half // 2}
        return {"side": side}

    def beside(d, axis, h):
        k = (1 << axis) ^ (PLANE * d)
        arrive((X, Y)[axis] + 2 * d + h, region(k, h))

    def across_x(d):
        k, rows_at = 2 ^ (PLANE * d), corner_rows(d, 0)
        start(copy(XD + d, region(k, **rows_at), region(k ^ 1, **rows_at), x_peer))

    def across_y(d):
        k, rows_at = 1 ^ (PLANE * d), corner_rows(d, 1)
        start(copy(YD + d, region(k, **rows_at), region(k ^ 2, **rows_at), y_peer))

    def above(flip):
        start(copy(B + flip, region(flip, 1), region(flip ^ PLANE, 1), near))

    def above_if(where, flip):
        @pl.when(where)
        def _():
            copy(B + flip, region(flip, 1), region(flip ^ PLANE, 1), near).start()

    def corner(d):
        k = 3 ^ (PLANE * d)
        arrive(XD + d, region(k, **corner_rows(d, 0)))
        arrive(YD + d, region(k, **corner_rows(d, 1)))

    def corner_joined(d):
        k = 3 ^ (PLANE * d)
        for number, side in ((XD, 0), (YD, 1)):
            joined(number + d, region(k, of=1 - core, **corner_rows(d, side)))

    def half_joined(number, k, h):
        joined(number + h, region(k, h, 1 - core))

    lane_r = lax.broadcasted_iota(jnp.int32, (count, count), 0)
    lane_c = lax.broadcasted_iota(jnp.int32, (count, count), 1)
    upper = (lane_r <= lane_c).astype(f32).astype(bf16)
    slot = lax.broadcasted_iota(jnp.int32, (slots, count), 0).astype(f32)

    def across(a, b):
        return lax.dot_general(a, b, (((1,), (1,)), ((), ())), preferred_element_type=f32)

    def block(k):
        return pl.ds(pl.multiple_of(k * count, count), count)

    width = out.shape[1]

    def halves():
        for target, which in ((other, 1 - core), (acc, core)):
            yield target, pl.ds(pl.multiple_of(which * width, width), width)

    def routed(ks):
        picks = []
        for b, k in enumerate(ks):
            match = all_ids[k] == me
            value = jnp.sum(jnp.where(match, all_gains[k], 0.0), axis=0, keepdims=True)
            chosen = jnp.sum(match.astype(f32), axis=0, keepdims=True)
            chosen = jnp.broadcast_to(chosen, (8, count))
            rank = jnp.dot(chosen.astype(bf16), upper, preferred_element_type=f32)
            where = jnp.where(chosen > 0.0, rank - 1.0, -1.0)[0:1]
            pick = (jnp.broadcast_to(where, (slots, count)) == slot).astype(f32)
            picks.append(pick)
            place = pl.ds(b * slots, slots)
            slot_w[place] = jnp.sum(pick * value, axis=1, keepdims=True)
            rows[place] = jnp.dot(
                pick.astype(bf16), every[block(k)], preferred_element_type=f32
            ).astype(bf16)
        live = pl.ds(0, len(ks) * slots)
        gate_part = across(rows[live], w_gate[...])
        up_part = across(rows[live], w_up[...])
        hidden = (jax.nn.silu(gate_part) * up_part * slot_w[live]).astype(bf16)
        for b, k in enumerate(ks):
            back = jnp.dot(
                picks[b].T.astype(bf16),
                hidden[b * slots : (b + 1) * slots],
                preferred_element_type=f32,
            )
            both[block(k)] = back.astype(bf16)
            for target, columns in halves():
                target[block(k)] = jnp.dot(
                    both[block(k)], w_down[:, columns], preferred_element_type=f32
                ).astype(bf16)

    def partials(at):
        pre = jnp.dot(every[at], all_in[...], preferred_element_type=f32)
        shared = (jax.nn.silu(pre[:, :LANES]) * pre[:, LANES:]).astype(bf16)
        for target, columns in halves():
            part = jnp.dot(shared, w_out[0:LANES, columns], preferred_element_type=f32)
            target[at] = (target[at].astype(f32) + part).astype(bf16)

    second = jnp.where(inner, 3, 2)
    third = 5 - second
    EARLY = []
    send_shared(EARLY)

    @pl.when(my_piece < pieces)
    def _():
        items = [
            pltpu.make_async_copy(source, target, local.at[2 + i])
            for i, (source, target) in enumerate(zip(parts(my_piece), places(me)))
        ]
        for item in items:
            item.start()
        for item in items:
            item.wait()

    @pl.when(my_piece >= pieces)
    def _():
        all_in[...] = jnp.zeros_like(all_in)
        w_out[0:LANES] = jnp.zeros((LANES, w_out.shape[1]), bf16)

    outer = jnp.logical_not(inner)
    for h in range(2):
        stage(1, h)
        start_inner(copy(Z + 4 + h, region(PLANE, h), region(2 * PLANE, h), far, E + 2 + h))
        if h:
            place = region(PLANE, h)
            start(copy(T + Z + 2 + h, place, place, twin))
        else:
            spread(1, h)
        back = copy(Z + 4 + h, region(3 * PLANE, h), region(2 * PLANE, h), near, E + 4 + h)
        stage_if(inner, 3, h, [back])
        beside(0, 0, h)
        beside(0, 1, h)
        if h:
            across_y(0)
            above_if(outer, 1)
            above_if(outer, 2)
        else:
            across_x(0)
    for k in range(1, wide):
        landed(G + k, all_ids.at[k])
        landed(G + wide + k, all_gains.at[k])
    for item in loads:
        item.wait()
    own.wait()
    for h in range(2):
        half_joined(Z + 2, PLANE, h)
        half_joined(X, 1, h)
        half_joined(Y, 2, h)
    for h in range(2):
        stage_if(outer, 2, h)
    beside(1, 0, 0)
    across_y(1)
    beside(1, 1, 0)
    across_x(1)
    for h in range(2):
        more = copy(Z + 6 + h, region(2 * PLANE, h), region(3 * PLANE, h), near, E + 6 + h)
        stage_if(inner, 2, h, [more])
    above_if(inner, 1)
    above_if(inner, 2)
    corner(0)
    above(3)
    routed([0, 1, 2, PLANE])
    send_shared([12, 8, 13, 9, 14, 10, 15, 11])
    for h in range(2):
        stage_if(outer, 3, h)
    for h in range(2):
        beside(second, 0, h)
        beside(second, 1, h)
        if h:
            across_y(second)
        else:
            across_x(second)
    send_shared([5, 6, 7, 4, 3, 1, 2])
    arrive(B + 1, region(1 ^ PLANE, 1))
    arrive(B + 2, region(2 ^ PLANE, 1))
    for h in range(2):
        half_joined(Z + 2 * second, PLANE * second, h)
    half_joined(X + 2, PLANE ^ 1, 0)
    half_joined(Y + 2, PLANE ^ 2, 0)
    joined(B + 1, region(1 ^ PLANE, 1, 1 - core))
    joined(B + 2, region(2 ^ PLANE, 1, 1 - core))
    corner_joined(0)
    routed([PLANE * second, PLANE ^ 1, PLANE ^ 2, 3])
    corner(1)
    arrive(B + 3, region(3 ^ PLANE, 1))
    for h in range(2):
        beside(third, 0, h)
        beside(third, 1, h)
        if h:
            across_y(third)
        else:
            across_x(third)
    for h in range(2):
        half_joined(Z + 2 * third, PLANE * third, h)
        half_joined(X + 2 * second, (PLANE * second) ^ 1, h)
        half_joined(Y + 2 * second, (PLANE * second) ^ 2, h)
    corner_joined(1)
    joined(B + 3, region(3 ^ PLANE, 1, 1 - core))
    routed([PLANE * third, (PLANE * second) ^ 1, (PLANE * second) ^ 2, 3 ^ PLANE])
    RT, RXD, RYD = R, R + wide, R + wide + lines
    RX, RY, RZ = RYD + lines, RYD + 2 * lines, RC
    RB = RZ + 10
    step = 16

    def rows_of(ref, k, begin=0, size=count):
        return ref.at[pl.ds(k * count + begin, size)]

    def add(target, sources):
        def one(i, carry):
            at = pl.ds(pl.multiple_of(i * step, step), step)
            value = target[at].astype(f32)
            for source in sources:
                value += source[at].astype(f32)
            target[at] = value.astype(bf16)
            return carry

        lax.fori_loop(0, target.shape[0] // step, one, 0)

    def compute(d, flips):
        first = PLANE * d + flips[0]
        partials(pl.ds(first * count, len(flips) * count))
        for flip in flips:
            k = PLANE * d + flip
            start(copy(RT + k, rows_of(other, k), rows_of(twin_in, k), twin))

    def fold(k):
        landed(RT + k, rows_of(twin_in, k))
        add(rows_of(acc, k), [rows_of(twin_in, k)])

    def cut(d):
        low = (0,) + tuple(count // part for part in (4, 4, 4))
        low = low[d]
        return low, (count - low) // 2

    def by_line(flip, d):
        low, number = cut(d)[0], 3 * (flip - 1) + d - 1
        if not low:
            return
        start(
            copy(
                RB + number,
                rows_of(acc, flip ^ (PLANE * d), 0, low),
                plane_in.at[number, pl.ds(0, low)],
                (me ^ (PLANE * d), core),
            )
        )

    def from_line(flip):
        for d in range(1, lines):
            low, number = cut(d)[0], 3 * (flip - 1) + d - 1
            if low:
                place = plane_in.at[number, pl.ds(0, low)]
                landed(RB + number, place)
                add(rows_of(acc, flip, 0, low), [place])

    def diagonal(d):
        k = 3 ^ (PLANE * d)
        low, tall = cut(d)
        fold(k)
        if d:
            by_line(3, d)
        else:
            from_line(3)
        place = pl.ds(0, tall)
        start(copy(RXD + d, rows_of(acc, k, low, tall), diag_in.at[0, d, place], x_peer))
        start(copy(RYD + d, rows_of(acc, k, low + tall, tall), diag_in.at[1, d, place], y_peer))

    def sides(d):
        low, tall = cut(d)
        place, rest = pl.ds(0, tall), pl.ds(low, 2 * tall)
        for flip in (2, 1):
            fold(flip ^ (PLANE * d))
            if d:
                by_line(flip, d)
            else:
                from_line(flip)
        k = 2 ^ (PLANE * d)
        landed(RXD + d, diag_in.at[0, d, place])
        add(rows_of(acc, k, low, tall), [diag_in.at[0, d, place]])
        start(copy(RY + d, rows_of(acc, k, low, 2 * tall), side_in.at[1, d, rest], y_peer))
        k = 1 ^ (PLANE * d)
        landed(RYD + d, diag_in.at[1, d, place])
        add(rows_of(acc, k, low + tall, tall), [diag_in.at[1, d, place]])
        start(copy(RX + d, rows_of(acc, k, low, 2 * tall), side_in.at[0, d, rest], x_peer))

    near_in, far_in, far_out = line_in.at[0], line_in.at[1], line_in.at[2]

    def upright(d):
        k = PLANE * d
        low, tall = cut(d)
        rest = pl.ds(low, 2 * tall)
        fold(k)
        landed(RX + d, side_in.at[0, d, rest])
        landed(RY + d, side_in.at[1, d, rest])
        add(rows_of(acc, k, low, 2 * tall), [side_in.at[0, d, rest], side_in.at[1, d, rest]])

    def legs(number, k, place, to):
        size = count // 2
        return [
            copy(
                RZ + 2 * number + h,
                rows_of(acc, k, h * size, size),
                place.at[pl.ds(h * size, size)],
                to,
            )
            for h in range(2)
        ]

    def outward(number, k, place):
        for item in legs(number, k, place, near):
            outer_started.append(item)

            @pl.when(outer)
            def _():
                item.start()

    def inward(number, place, k, items):
        inner_started.extend(items)
        size = count // 2

        @pl.when(inner)
        def _():
            for h, item in enumerate(items):
                part = place.at[pl.ds(h * size, size)]
                landed(RZ + 2 * number + h, part)
                add(rows_of(acc, k, h * size, size), [part])
                item.start()

    def leg_landed(number, place):
        size = count // 2
        for h in range(2):
            landed(RZ + 2 * number + h, place.at[pl.ds(h * size, size)])

    one, two, three = PLANE, 2 * PLANE, 3 * PLANE
    for h in range(2):
        half_joined(X + 2 * third, (PLANE * third) ^ 1, h)
        half_joined(Y + 2 * third, (PLANE * third) ^ 2, h)
    routed([(PLANE * third) ^ 1, (PLANE * third) ^ 2])
    corner(second)
    corner(third)
    corner_joined(second)
    corner_joined(third)
    routed([3 ^ (PLANE * second), 3 ^ (PLANE * third)])
    for k in range(1, wide):

        @pl.when(my_piece < pieces)
        def _():
            for i, target in enumerate(places(me ^ k)):
                landed(W + k + i * wide, target)

    compute(3, [3])
    compute(2, [3])
    diagonal(3)
    compute(3, [1, 2])
    diagonal(2)
    compute(3, [0])
    compute(1, [3])
    sides(3)
    diagonal(1)
    compute(2, [1, 2])
    compute(2, [0])
    sides(2)
    upright(3)
    outward(0, three, near_in)
    compute(0, [3])
    diagonal(0)
    compute(1, [1, 2])
    sides(1)
    upright(2)
    outward(1, two, far_in)
    compute(1, [0])
    inward(0, near_in, two, legs(2, two, far_out, far))
    compute(0, [1, 2])
    sides(0)
    upright(1)
    outward(4, one, line_in.at[4])
    compute(0, [0])
    inward(1, far_in, three, legs(3, three, line_in.at[3], far))
    inward(2, far_out, one, legs(4, one, line_in.at[4], near))
    upright(0)

    @pl.when(inner)
    def _():
        leg_landed(3, line_in.at[3])
        add(rows_of(acc, 0), [line_in.at[3]])

    leg_landed(4, line_in.at[4])

    def last(i, carry):
        at = pl.ds(pl.multiple_of(i * step, step), step)
        value = acc[at].astype(f32)
        out[at] = (value + line_in[4, at].astype(f32)).astype(bf16)
        return carry

    lax.fori_loop(0, count // step, last, 0)
    for k in range(1, wide):

        @pl.when(piece_table(wide, pieces, core, me ^ k) < pieces)
        def _():
            for item in shared_copies(k):
                item.wait_send()

    for item in started:
        item.wait_send()

    for h in range(2):
        for item in onward(second, h) + onward(third, h):
            item.wait_send()
    for flip in (1, 2):
        copy(B + flip, region(flip, 1), region(flip ^ PLANE, 1), near).wait_send()

    @pl.when(inner)
    def _():
        for h in range(2):
            back = copy(Z + 4 + h, region(3 * PLANE, h), region(2 * PLANE, h), near, E + 4 + h)
            back.wait_send()
            more = copy(Z + 6 + h, region(2 * PLANE, h), region(3 * PLANE, h), near, E + 6 + h)
            more.wait_send()
        for item in inner_started:
            item.wait_send()

    @pl.when(jnp.logical_not(inner))
    def _():
        for item in outer_started:
            item.wait_send()


def fused(wide, narrow, slots, tokens, ids, gains, gate, up, down, w_gate, w_up, w_down):
    count, width = tokens.shape
    part = width // narrow
    lines = wide // PLANE
    total = wide * count
    sems = 22 * lines + 6 * wide + 10 + 9 + 8
    bf16, f32 = jnp.bfloat16, jnp.float32
    return pl.pallas_call(
        functools.partial(fused_kernel, wide, slots),
        out_shape=jax.ShapeDtypeStruct((count, part), bf16),
        in_specs=[VMEM] * 6 + [ANY] * 3,
        out_specs=VMEM,
        scratch_shapes=[
            pltpu.VMEM((total, width), bf16),
            pltpu.VMEM((wide * gate.shape[0], 2 * LANES), bf16),
            pltpu.VMEM((wide,) + ids.shape, jnp.int32),
            pltpu.VMEM((wide,) + gains.shape, f32),
            pltpu.VMEM(w_gate.shape, bf16),
            pltpu.VMEM(w_up.shape, bf16),
            pltpu.VMEM((LANES + w_down.shape[0], w_down.shape[1]), bf16),
            pltpu.VMEM((lines * slots, width), bf16),
            pltpu.VMEM((lines * slots, 1), f32),
            pltpu.VMEM((total, w_gate.shape[0]), bf16),
            pltpu.VMEM((total, part), bf16),
            pltpu.VMEM((total, part), bf16),
            pltpu.VMEM((total, part), bf16),
            pltpu.VMEM((2, lines, count // 2, part), bf16),
            pltpu.VMEM((2, lines, count, part), bf16),
            pltpu.VMEM((5, count, part), bf16),
            pltpu.VMEM((3 * (lines - 1), count // 2, part), bf16),
            pltpu.SemaphoreType.DMA((sems,)),
            pltpu.SemaphoreType.DMA((sems,)),
            pltpu.SemaphoreType.DMA((9,)),
        ],
        compiler_params=pltpu.CompilerParams(
            collective_id=0, has_side_effects=True, vmem_limit_bytes=63 << 20
        ),
    )(tokens, ids, gains, gate, up, down, w_gate, w_up, w_down)


def gather_body(
    tokens,
    expert_ids,
    gate_weights,
    shared_gate,
    shared_up,
    shared_down,
    expert_gate,
    expert_up,
    expert_down,
):
    tok_count, top_count = expert_ids.shape
    wide = lax.axis_size("wide")
    narrow = lax.axis_size("narrow")
    experts = wide * expert_gate.shape[0]
    capacity, _ = plan(tok_count, top_count, experts, wide)
    return fused(
        wide,
        narrow,
        capacity,
        tokens,
        expert_ids.T,
        gate_weights.T,
        shared_gate,
        shared_up,
        shared_down,
        expert_gate[0].T,
        expert_up[0].T,
        expert_down[0],
    )


def solution(mesh):
    in_specs = (
        P("wide", None),
        P("wide", None),
        P("wide", None),
        P("wide", "narrow"),
        P("wide", "narrow"),
        P("narrow", "wide"),
        P("wide", None, "narrow"),
        P("wide", None, "narrow"),
        P("wide", "narrow", None),
    )
    out_specs = P("wide", "narrow")
    wide_count = mesh.shape["wide"]

    def body(*args):
        tok_count, top_count = args[1].shape
        gathers = plan(tok_count, top_count, wide_count * args[6].shape[0], wide_count)[1]
        return (gather_body if gathers else dispatch_body)(*args)

    return jax.shard_map(body, mesh=mesh, in_specs=in_specs, out_specs=out_specs, check_vma=False)
```

```python
import functools

import jax
import jax.numpy as jnp
from jax import lax
from jax.experimental import pallas as pl
from jax.experimental.pallas import tpu as pltpu
from jax.sharding import PartitionSpec as P


def expert_ffn(received, w_gate, w_up, w_down):
    senders, items, width = received.shape
    flat_rows = received.reshape(senders * items, width)
    gate_part = jnp.dot(flat_rows, w_gate, preferred_element_type=jnp.float32)
    up_part = jnp.dot(flat_rows, w_up, preferred_element_type=jnp.float32)
    hidden = (jax.nn.silu(gate_part) * up_part).astype(jnp.bfloat16)
    partial_value = jnp.dot(hidden, w_down, preferred_element_type=jnp.float32).astype(jnp.bfloat16)
    return partial_value.reshape(senders, items, w_down.shape[1])


def dispatch_body(
    tokens,
    expert_ids,
    gate_weights,
    shared_gate,
    shared_up,
    shared_down,
    expert_gate,
    expert_up,
    expert_down,
):
    tok_count, width = tokens.shape
    top_count = expert_ids.shape[1]
    experts = lax.axis_size("wide") * expert_gate.shape[0]
    capacity = min(tok_count, 4 * tok_count * top_count // (3 * experts))
    narrow_count = lax.axis_size("narrow")
    w_gate = expert_gate[0]
    w_up = expert_up[0]
    w_down = expert_down[0]
    pairs = tok_count * top_count
    flat_ids = expert_ids.reshape(pairs)
    onehot = (flat_ids[:, None] == jnp.arange(experts, dtype=jnp.int32)[None, :]).astype(jnp.int32)
    before = jnp.cumsum(onehot, axis=0) - onehot
    slot_pos = jnp.sum(before * onehot, axis=1)
    target_slot = flat_ids * capacity + slot_pos
    source = (
        jnp.full((experts * capacity,), -1, jnp.int32)
        .at[target_slot]
        .set(jnp.arange(pairs, dtype=jnp.int32))
    )
    filled = source >= 0
    token_of = jnp.where(filled, source // top_count, 0)
    outgoing = jnp.where(filled[:, None], tokens[token_of], jnp.zeros((), jnp.bfloat16))
    outgoing = outgoing.reshape(experts, capacity, width)
    quarter = capacity // narrow_count
    own_rows = lax.dynamic_slice_in_dim(outgoing, lax.axis_index("narrow") * quarter, quarter, 1)
    arrived = lax.all_to_all(own_rows, "wide", split_axis=0, concat_axis=0, tiled=True)
    joined = lax.all_gather(arrived, "narrow", axis=1, tiled=True)
    partial_value = expert_ffn(joined, w_gate, w_up, w_down)
    expert_out = (
        lax.psum_scatter(partial_value, "narrow", scatter_dimension=2, tiled=True)
        .astype(jnp.float32)
        .astype(jnp.bfloat16)
    )
    returned = lax.all_to_all(expert_out, "wide", split_axis=0, concat_axis=0, tiled=True)
    returned_rows = returned.reshape(experts * capacity, returned.shape[2])
    pair_rows = returned_rows[target_slot].astype(jnp.float32)
    weighted = gate_weights.reshape(pairs, 1) * pair_rows
    routed = jnp.sum(weighted.reshape(tok_count, top_count, returned.shape[2]), axis=1)
    gate_sum = jnp.dot(
        tokens,
        lax.all_gather(shared_gate, "wide", axis=0, tiled=True),
        preferred_element_type=jnp.float32,
    )
    up_sum = jnp.dot(
        tokens,
        lax.all_gather(shared_up, "wide", axis=0, tiled=True),
        preferred_element_type=jnp.float32,
    )
    shared_hidden = (jax.nn.silu(gate_sum) * up_sum).astype(jnp.bfloat16)
    shared_terms = jnp.dot(
        shared_hidden,
        lax.all_gather(shared_down, "wide", axis=1, tiled=True),
        preferred_element_type=jnp.float32,
    )
    shared = lax.psum_scatter(shared_terms, "narrow", scatter_dimension=1, tiled=True)
    return (shared + routed).astype(jnp.bfloat16)


MESH = pl.DeviceIdType.MESH
ANY = pl.BlockSpec(memory_space=pl.ANY)
VMEM = pl.BlockSpec(memory_space=pltpu.VMEM)
LANES = 128
PLANE = 4


def plan(tok_count, top_count, experts, wide_count):
    capacity = min(tok_count, 4 * tok_count * top_count // (3 * experts))
    return capacity, wide_count == PLANE**2 and wide_count * tok_count <= 4 * experts * capacity


def homes(wide, pieces, core):
    lines = wide // PLANE
    inner, edge, late = [], [], []
    for z in range(lines):
        pair = [PLANE * z + i for i in ((1, 2) if z % 2 else (0, 3))]
        if 0 < z < lines - 1:
            inner += pair
        else:
            edge.append(pair[0])
            late.append(pair[1])
    both = (inner + edge + late)[: max(0, 2 * pieces - wide)]
    single = [chip for chip in range(wide) if chip not in both]
    return (both + single[core::2])[:pieces]


def piece_table(wide, pieces, core, chip):
    bits = pieces.bit_length()
    per = 30 // bits
    words = []
    for which in range(2):
        held = homes(wide, pieces, which)
        row = [held.index(j) if j in held else pieces for j in range(wide)]
        words.append(
            [
                sum(v << (bits * i) for i, v in enumerate(row[at : at + per]))
                for at in range(0, wide, per)
            ]
        )
    word = jnp.int32(0)
    for i, (low, high) in enumerate(zip(*words)):
        word = jnp.where(chip // per == i, jnp.where(core == 0, low, high), word)
    return (word >> (bits * (chip % per))) & ((1 << bits) - 1)


def greet(devices):
    barrier = pltpu.get_barrier_semaphore()
    for device in devices:
        pl.semaphore_signal(barrier, inc=1, device_id=device, device_id_type=MESH)
    pl.semaphore_wait(barrier, len(devices))


def fused_kernel(
    wide,
    slots,
    tok,
    ids,
    gains,
    gate,
    up,
    down,
    w_gate_in,
    w_up_in,
    w_down_in,
    out,
    every,
    all_in,
    all_ids,
    all_gains,
    w_gate,
    w_up,
    w_out,
    rows,
    slot_w,
    both,
    other,
    acc,
    twin_in,
    diag_in,
    side_in,
    line_in,
    plane_in,
    send,
    recv,
    local,
):
    f32, bf16 = jnp.float32, jnp.bfloat16
    me = lax.axis_index("wide")
    core = lax.axis_index("narrow")
    lines = wide // PLANE
    count = tok.shape[0]
    share = count // 2
    half = share // 2
    pieces = gate.shape[1] // LANES
    my_piece = piece_table(wide, pieces, core, me)
    greet([(me ^ k, core) for k in range(1, wide)] + [(me, 1 - core)])
    x_peer, y_peer, twin = (me ^ 1, core), (me ^ 2, core), (me, 1 - core)
    plane = me // PLANE
    inner = (plane > 0) & (plane < lines - 1)
    started = []
    inner_started = []
    outer_started = []

    def copy(number, source, target, device, sent=None):
        return pltpu.make_async_remote_copy(
            src_ref=source,
            dst_ref=target,
            send_sem=send.at[number if sent is None else sent],
            recv_sem=recv.at[number],
            device_id=device,
            device_id_type=MESH,
        )

    def start(item):
        item.start()
        started.append(item)

    def start_inner(item):
        inner_started.append(item)

        @pl.when(inner)
        def _():
            item.start()

    def landed(number, place):
        copy(number, place, place, twin).wait_recv()

    def region(k, side=None, of=core, begin=0, size=None):
        first = k * count + of * share
        if size is not None:
            first, tile, size = first + begin, LANES // 8, size
        elif side is None:
            tile = size = share
        else:
            first, tile, size = first + side * half, half, half
        return every.at[pl.ds(pl.multiple_of(first, tile), size)]

    Z, X, Y, XD, YD, B = 0, 2 * lines, 4 * lines, 6 * lines, 7 * lines, 8 * lines
    T = 9 * lines
    W = 2 * T
    G = W + 3 * wide
    R = G + 2 * wide
    RC = R + wide + 4 * lines
    E = RC + 10 + 9

    def arrive(number, place):
        landed(number, place)
        start(copy(T + number, place, place, twin))

    def joined(number, place):
        landed(T + number, place)

    own = pltpu.make_async_copy(tok, every.at[pl.ds(0, count)], local.at[0])
    own.start()
    near, far = (me ^ PLANE, core), (me ^ (3 * PLANE), core)
    for h in range(2):
        mine = tok.at[pl.ds(pl.multiple_of(core * share + h * half, half), half)]
        start(copy(Z + 2 + h, mine, region(PLANE, h), near))
        start_inner(copy(Z + 6 + h, mine, region(3 * PLANE, h), far, E + h))
        start(copy(X + h, mine, region(1, h), x_peer))
        start(copy(Y + h, mine, region(2, h), y_peer))
    for k in range(1, wide):
        start(copy(G + k, ids, all_ids.at[k], (me ^ k, core)))
        start(copy(G + wide + k, gains, all_gains.at[k], (me ^ k, core)))
    loads = [
        pltpu.make_async_copy(ids, all_ids.at[0], local.at[1]),
        pltpu.make_async_copy(gains, all_gains.at[0], local.at[8]),
    ]
    w_down = w_out.at[pl.ds(LANES, w_down_in.shape[0])]
    for number, (source, target) in enumerate(
        ((w_gate_in, w_gate), (w_up_in, w_up), (w_down_in, w_down))
    ):
        loads.append(pltpu.make_async_copy(source, target, local.at[5 + number]))
    for item in loads:
        item.start()

    def places(chip):
        at = pl.ds(pl.multiple_of(chip * LANES, LANES), LANES)
        return (
            all_in.at[at, pl.ds(0, LANES)],
            all_in.at[at, pl.ds(LANES, LANES)],
            w_out.at[pl.ds(0, LANES), at],
        )

    def parts(piece):
        piece = jnp.minimum(piece, pieces - 1)
        part = pl.ds(pl.multiple_of(piece * LANES, LANES), LANES)
        return (gate.at[:, part], up.at[:, part], down.at[part])

    def shared_copies(k):
        piece = piece_table(wide, pieces, core, me ^ k)
        return [
            copy(W + k + i * wide, source, target, (me ^ k, core))
            for i, (source, target) in enumerate(zip(parts(piece), places(me)))
        ]

    def send_shared(ks):
        for k in ks:

            @pl.when(piece_table(wide, pieces, core, me ^ k) < pieces)
            def _():
                for item in shared_copies(k):
                    item.start()

    def onward(d, h):
        place = region(PLANE * d, h)
        return [
            copy(X + 2 * d + h, place, region((PLANE * d) ^ 1, h), x_peer),
            copy(Y + 2 * d + h, place, region((PLANE * d) ^ 2, h), y_peer),
            copy(T + Z + 2 * d + h, place, place, twin),
        ]

    def stage(d, h):
        landed(Z + 2 * d + h, region(PLANE * d, h))

    def stage_if(where, d, h, then=()):
        @pl.when(where)
        def _():
            stage(d, h)
            for item in list(then) + onward(d, h):
                item.start()

    def spread(d, h):
        for item in onward(d, h):
            start(item)

    def corner_rows(d, side):
        if isinstance(d, int) and d == 1:
            return {"begin": side * (half // 2), "size": half // 2}
        return {"side": side}

    def beside(d, axis, h):
        k = (1 << axis) ^ (PLANE * d)
        arrive((X, Y)[axis] + 2 * d + h, region(k, h))

    def across_x(d):
        k, rows_at = 2 ^ (PLANE * d), corner_rows(d, 0)
        start(copy(XD + d, region(k, **rows_at), region(k ^ 1, **rows_at), x_peer))

    def across_y(d):
        k, rows_at = 1 ^ (PLANE * d), corner_rows(d, 1)
        start(copy(YD + d, region(k, **rows_at), region(k ^ 2, **rows_at), y_peer))

    def above(flip):
        start(copy(B + flip, region(flip, 1), region(flip ^ PLANE, 1), near))

    def above_if(where, flip):
        @pl.when(where)
        def _():
            copy(B + flip, region(flip, 1), region(flip ^ PLANE, 1), near).start()

    def corner(d):
        k = 3 ^ (PLANE * d)
        arrive(XD + d, region(k, **corner_rows(d, 0)))
        arrive(YD + d, region(k, **corner_rows(d, 1)))

    def corner_joined(d):
        k = 3 ^ (PLANE * d)
        for number, side in ((XD, 0), (YD, 1)):
            joined(number + d, region(k, of=1 - core, **corner_rows(d, side)))

    def half_joined(number, k, h):
        joined(number + h, region(k, h, 1 - core))

    lane_r = lax.broadcasted_iota(jnp.int32, (count, count), 0)
    lane_c = lax.broadcasted_iota(jnp.int32, (count, count), 1)
    upper = (lane_r <= lane_c).astype(f32).astype(bf16)
    slot = lax.broadcasted_iota(jnp.int32, (slots, count), 0).astype(f32)

    def across(a, b):
        return lax.dot_general(a, b, (((1,), (1,)), ((), ())), preferred_element_type=f32)

    def block(k):
        return pl.ds(pl.multiple_of(k * count, count), count)

    width = out.shape[1]

    def halves():
        for target, which in ((other, 1 - core), (acc, core)):
            yield target, pl.ds(pl.multiple_of(which * width, width), width)

    def routed(ks):
        picks = []
        for b, k in enumerate(ks):
            match = all_ids[k] == me
            value = jnp.sum(jnp.where(match, all_gains[k], 0.0), axis=0, keepdims=True)
            chosen = jnp.sum(match.astype(f32), axis=0, keepdims=True)
            chosen = jnp.broadcast_to(chosen, (8, count))
            rank = jnp.dot(chosen.astype(bf16), upper, preferred_element_type=f32)
            where = jnp.where(chosen > 0.0, rank - 1.0, -1.0)[0:1]
            pick = (jnp.broadcast_to(where, (slots, count)) == slot).astype(f32)
            picks.append(pick)
            place = pl.ds(b * slots, slots)
            slot_w[place] = jnp.sum(pick * value, axis=1, keepdims=True)
            rows[place] = jnp.dot(
                pick.astype(bf16), every[block(k)], preferred_element_type=f32
            ).astype(bf16)
        live = pl.ds(0, len(ks) * slots)
        gate_part = across(rows[live], w_gate[...])
        up_part = across(rows[live], w_up[...])
        hidden = (jax.nn.silu(gate_part) * up_part * slot_w[live]).astype(bf16)
        for b, k in enumerate(ks):
            back = jnp.dot(
                picks[b].T.astype(bf16),
                hidden[b * slots : (b + 1) * slots],
                preferred_element_type=f32,
            )
            both[block(k)] = back.astype(bf16)
            for target, columns in halves():
                target[block(k)] = jnp.dot(
                    both[block(k)], w_down[:, columns], preferred_element_type=f32
                ).astype(bf16)

    def partials(at):
        pre = jnp.dot(every[at], all_in[...], preferred_element_type=f32)
        shared = (jax.nn.silu(pre[:, :LANES]) * pre[:, LANES:]).astype(bf16)
        for target, columns in halves():
            part = jnp.dot(shared, w_out[0:LANES, columns], preferred_element_type=f32)
            target[at] = (target[at].astype(f32) + part).astype(bf16)

    second = jnp.where(inner, 3, 2)
    third = 5 - second
    EARLY = []
    send_shared(EARLY)

    @pl.when(my_piece < pieces)
    def _():
        items = [
            pltpu.make_async_copy(source, target, local.at[2 + i])
            for i, (source, target) in enumerate(zip(parts(my_piece), places(me)))
        ]
        for item in items:
            item.start()
        for item in items:
            item.wait()

    @pl.when(my_piece >= pieces)
    def _():
        all_in[...] = jnp.zeros_like(all_in)
        w_out[0:LANES] = jnp.zeros((LANES, w_out.shape[1]), bf16)

    outer = jnp.logical_not(inner)
    for h in range(2):
        stage(1, h)
        start_inner(copy(Z + 4 + h, region(PLANE, h), region(2 * PLANE, h), far, E + 2 + h))
        if h:
            place = region(PLANE, h)
            start(copy(T + Z + 2 + h, place, place, twin))
        else:
            spread(1, h)
        back = copy(Z + 4 + h, region(3 * PLANE, h), region(2 * PLANE, h), near, E + 4 + h)
        stage_if(inner, 3, h, [back])
        beside(0, 0, h)
        beside(0, 1, h)
        if h:
            across_y(0)
            above_if(outer, 1)
            above_if(outer, 2)
        else:
            across_x(0)
    for k in range(1, wide):
        landed(G + k, all_ids.at[k])
        landed(G + wide + k, all_gains.at[k])
    for item in loads:
        item.wait()
    own.wait()
    for h in range(2):
        half_joined(Z + 2, PLANE, h)
        half_joined(X, 1, h)
        half_joined(Y, 2, h)
    for h in range(2):
        stage_if(outer, 2, h)
    beside(1, 0, 0)
    across_y(1)
    beside(1, 1, 0)
    across_x(1)
    for h in range(2):
        more = copy(Z + 6 + h, region(2 * PLANE, h), region(3 * PLANE, h), near, E + 6 + h)
        stage_if(inner, 2, h, [more])
    above_if(inner, 1)
    above_if(inner, 2)
    corner(0)
    above(3)
    routed([0, 1, 2, PLANE])
    send_shared([12, 8, 13, 9, 14, 10, 15, 11])
    for h in range(2):
        stage_if(outer, 3, h)
    for h in range(2):
        beside(second, 0, h)
        beside(second, 1, h)
        if h:
            across_y(second)
        else:
            across_x(second)
    send_shared([5, 6, 7, 4, 3, 1, 2])
    arrive(B + 1, region(1 ^ PLANE, 1))
    arrive(B + 2, region(2 ^ PLANE, 1))
    for h in range(2):
        half_joined(Z + 2 * second, PLANE * second, h)
    half_joined(X + 2, PLANE ^ 1, 0)
    half_joined(Y + 2, PLANE ^ 2, 0)
    joined(B + 1, region(1 ^ PLANE, 1, 1 - core))
    joined(B + 2, region(2 ^ PLANE, 1, 1 - core))
    corner_joined(0)
    routed([PLANE * second, PLANE ^ 1, PLANE ^ 2, 3])
    corner(1)
    arrive(B + 3, region(3 ^ PLANE, 1))
    for h in range(2):
        beside(third, 0, h)
        beside(third, 1, h)
        if h:
            across_y(third)
        else:
            across_x(third)
    for h in range(2):
        half_joined(Z + 2 * third, PLANE * third, h)
        half_joined(X + 2 * second, (PLANE * second) ^ 1, h)
        half_joined(Y + 2 * second, (PLANE * second) ^ 2, h)
    corner_joined(1)
    joined(B + 3, region(3 ^ PLANE, 1, 1 - core))
    routed([PLANE * third, (PLANE * second) ^ 1, (PLANE * second) ^ 2, 3 ^ PLANE])
    RT, RXD, RYD = R, R + wide, R + wide + lines
    RX, RY, RZ = RYD + lines, RYD + 2 * lines, RC
    RB = RZ + 10
    step = 16

    def rows_of(ref, k, begin=0, size=count):
        return ref.at[pl.ds(k * count + begin, size)]

    def add(target, sources):
        def one(i, carry):
            at = pl.ds(pl.multiple_of(i * step, step), step)
            value = target[at].astype(f32)
            for source in sources:
                value += source[at].astype(f32)
            target[at] = value.astype(bf16)
            return carry

        lax.fori_loop(0, target.shape[0] // step, one, 0)

    def compute(d, flips):
        first = PLANE * d + flips[0]
        partials(pl.ds(first * count, len(flips) * count))
        for flip in flips:
            k = PLANE * d + flip
            start(copy(RT + k, rows_of(other, k), rows_of(twin_in, k), twin))

    def fold(k):
        landed(RT + k, rows_of(twin_in, k))
        add(rows_of(acc, k), [rows_of(twin_in, k)])

    def cut(d):
        low = (0,) + tuple(count // part for part in (4, 4, 4))
        low = low[d]
        return low, (count - low) // 2

    def by_line(flip, d):
        low, number = cut(d)[0], 3 * (flip - 1) + d - 1
        if not low:
            return
        start(
            copy(
                RB + number,
                rows_of(acc, flip ^ (PLANE * d), 0, low),
                plane_in.at[number, pl.ds(0, low)],
                (me ^ (PLANE * d), core),
            )
        )

    def from_line(flip):
        for d in range(1, lines):
            low, number = cut(d)[0], 3 * (flip - 1) + d - 1
            if low:
                place = plane_in.at[number, pl.ds(0, low)]
                landed(RB + number, place)
                add(rows_of(acc, flip, 0, low), [place])

    def diagonal(d):
        k = 3 ^ (PLANE * d)
        low, tall = cut(d)
        fold(k)
        if d:
            by_line(3, d)
        else:
            from_line(3)
        place = pl.ds(0, tall)
        start(copy(RXD + d, rows_of(acc, k, low, tall), diag_in.at[0, d, place], x_peer))
        start(copy(RYD + d, rows_of(acc, k, low + tall, tall), diag_in.at[1, d, place], y_peer))

    def sides(d):
        low, tall = cut(d)
        place, rest = pl.ds(0, tall), pl.ds(low, 2 * tall)
        for flip in (2, 1):
            fold(flip ^ (PLANE * d))
            if d:
                by_line(flip, d)
            else:
                from_line(flip)
        k = 2 ^ (PLANE * d)
        landed(RXD + d, diag_in.at[0, d, place])
        add(rows_of(acc, k, low, tall), [diag_in.at[0, d, place]])
        start(copy(RY + d, rows_of(acc, k, low, 2 * tall), side_in.at[1, d, rest], y_peer))
        k = 1 ^ (PLANE * d)
        landed(RYD + d, diag_in.at[1, d, place])
        add(rows_of(acc, k, low + tall, tall), [diag_in.at[1, d, place]])
        start(copy(RX + d, rows_of(acc, k, low, 2 * tall), side_in.at[0, d, rest], x_peer))

    near_in, far_in, far_out = line_in.at[0], line_in.at[1], line_in.at[2]

    def upright(d):
        k = PLANE * d
        low, tall = cut(d)
        rest = pl.ds(low, 2 * tall)
        fold(k)
        landed(RX + d, side_in.at[0, d, rest])
        landed(RY + d, side_in.at[1, d, rest])
        add(rows_of(acc, k, low, 2 * tall), [side_in.at[0, d, rest], side_in.at[1, d, rest]])

    def legs(number, k, place, to):
        size = count // 2
        return [
            copy(
                RZ + 2 * number + h,
                rows_of(acc, k, h * size, size),
                place.at[pl.ds(h * size, size)],
                to,
            )
            for h in range(2)
        ]

    def outward(number, k, place):
        for item in legs(number, k, place, near):
            outer_started.append(item)

            @pl.when(outer)
            def _():
                item.start()

    def inward(number, place, k, items):
        inner_started.extend(items)
        size = count // 2

        @pl.when(inner)
        def _():
            for h, item in enumerate(items):
                part = place.at[pl.ds(h * size, size)]
                landed(RZ + 2 * number + h, part)
                add(rows_of(acc, k, h * size, size), [part])
                item.start()

    def leg_landed(number, place):
        size = count // 2
        for h in range(2):
            landed(RZ + 2 * number + h, place.at[pl.ds(h * size, size)])

    one, two, three = PLANE, 2 * PLANE, 3 * PLANE
    for h in range(2):
        half_joined(X + 2 * third, (PLANE * third) ^ 1, h)
        half_joined(Y + 2 * third, (PLANE * third) ^ 2, h)
    routed([(PLANE * third) ^ 1, (PLANE * third) ^ 2])
    corner(second)
    corner(third)
    corner_joined(second)
    corner_joined(third)
    routed([3 ^ (PLANE * second), 3 ^ (PLANE * third)])
    for k in range(1, wide):

        @pl.when(my_piece < pieces)
        def _():
            for i, target in enumerate(places(me ^ k)):
                landed(W + k + i * wide, target)

    compute(3, [3])
    compute(2, [3])
    diagonal(3)
    compute(3, [1, 2])
    diagonal(2)
    compute(3, [0])
    compute(1, [3])
    sides(3)
    diagonal(1)
    compute(2, [1, 2])
    compute(2, [0])
    sides(2)
    upright(3)
    outward(0, three, near_in)
    compute(0, [3])
    diagonal(0)
    compute(1, [1, 2])
    sides(1)
    upright(2)
    outward(1, two, far_in)
    inward(0, near_in, two, legs(2, two, far_out, far))
    compute(1, [0])
    compute(0, [1, 2])
    sides(0)
    upright(1)
    outward(4, one, line_in.at[4])
    compute(0, [0])
    inward(1, far_in, three, legs(3, three, line_in.at[3], far))
    inward(2, far_out, one, legs(4, one, line_in.at[4], near))
    upright(0)

    @pl.when(inner)
    def _():
        leg_landed(3, line_in.at[3])
        add(rows_of(acc, 0), [line_in.at[3]])

    leg_landed(4, line_in.at[4])

    def last(i, carry):
        at = pl.ds(pl.multiple_of(i * step, step), step)
        value = acc[at].astype(f32)
        out[at] = (value + line_in[4, at].astype(f32)).astype(bf16)
        return carry

    lax.fori_loop(0, count // step, last, 0)
    for k in range(1, wide):

        @pl.when(piece_table(wide, pieces, core, me ^ k) < pieces)
        def _():
            for item in shared_copies(k):
                item.wait_send()

    for item in started:
        item.wait_send()

    for h in range(2):
        for item in onward(second, h) + onward(third, h):
            item.wait_send()
    for flip in (1, 2):
        copy(B + flip, region(flip, 1), region(flip ^ PLANE, 1), near).wait_send()

    @pl.when(inner)
    def _():
        for h in range(2):
            back = copy(Z + 4 + h, region(3 * PLANE, h), region(2 * PLANE, h), near, E + 4 + h)
            back.wait_send()
            more = copy(Z + 6 + h, region(2 * PLANE, h), region(3 * PLANE, h), near, E + 6 + h)
            more.wait_send()
        for item in inner_started:
            item.wait_send()

    @pl.when(jnp.logical_not(inner))
    def _():
        for item in outer_started:
            item.wait_send()


def fused(wide, narrow, slots, tokens, ids, gains, gate, up, down, w_gate, w_up, w_down):
    count, width = tokens.shape
    part = width // narrow
    lines = wide // PLANE
    total = wide * count
    sems = 22 * lines + 6 * wide + 10 + 9 + 8
    bf16, f32 = jnp.bfloat16, jnp.float32
    return pl.pallas_call(
        functools.partial(fused_kernel, wide, slots),
        out_shape=jax.ShapeDtypeStruct((count, part), bf16),
        in_specs=[VMEM] * 6 + [ANY] * 3,
        out_specs=VMEM,
        scratch_shapes=[
            pltpu.VMEM((total, width), bf16),
            pltpu.VMEM((wide * gate.shape[0], 2 * LANES), bf16),
            pltpu.VMEM((wide,) + ids.shape, jnp.int32),
            pltpu.VMEM((wide,) + gains.shape, f32),
            pltpu.VMEM(w_gate.shape, bf16),
            pltpu.VMEM(w_up.shape, bf16),
            pltpu.VMEM((LANES + w_down.shape[0], w_down.shape[1]), bf16),
            pltpu.VMEM((lines * slots, width), bf16),
            pltpu.VMEM((lines * slots, 1), f32),
            pltpu.VMEM((total, w_gate.shape[0]), bf16),
            pltpu.VMEM((total, part), bf16),
            pltpu.VMEM((total, part), bf16),
            pltpu.VMEM((total, part), bf16),
            pltpu.VMEM((2, lines, count // 2, part), bf16),
            pltpu.VMEM((2, lines, count, part), bf16),
            pltpu.VMEM((5, count, part), bf16),
            pltpu.VMEM((3 * (lines - 1), count // 2, part), bf16),
            pltpu.SemaphoreType.DMA((sems,)),
            pltpu.SemaphoreType.DMA((sems,)),
            pltpu.SemaphoreType.DMA((9,)),
        ],
        compiler_params=pltpu.CompilerParams(
            collective_id=0, has_side_effects=True, vmem_limit_bytes=63 << 20
        ),
    )(tokens, ids, gains, gate, up, down, w_gate, w_up, w_down)


def gather_body(
    tokens,
    expert_ids,
    gate_weights,
    shared_gate,
    shared_up,
    shared_down,
    expert_gate,
    expert_up,
    expert_down,
):
    tok_count, top_count = expert_ids.shape
    wide = lax.axis_size("wide")
    narrow = lax.axis_size("narrow")
    experts = wide * expert_gate.shape[0]
    capacity, _ = plan(tok_count, top_count, experts, wide)
    return fused(
        wide,
        narrow,
        capacity,
        tokens,
        expert_ids.T,
        gate_weights.T,
        shared_gate,
        shared_up,
        shared_down,
        expert_gate[0].T,
        expert_up[0].T,
        expert_down[0],
    )


def solution(mesh):
    in_specs = (
        P("wide", None),
        P("wide", None),
        P("wide", None),
        P("wide", "narrow"),
        P("wide", "narrow"),
        P("narrow", "wide"),
        P("wide", None, "narrow"),
        P("wide", None, "narrow"),
        P("wide", "narrow", None),
    )
    out_specs = P("wide", "narrow")
    wide_count = mesh.shape["wide"]

    def body(*args):
        tok_count, top_count = args[1].shape
        gathers = plan(tok_count, top_count, wide_count * args[6].shape[0], wide_count)[1]
        return (gather_body if gathers else dispatch_body)(*args)

    return jax.shard_map(body, mesh=mesh, in_specs=in_specs, out_specs=out_specs, check_vma=False)
```
